32 devices in a mesh: patch: 8 (over y, x, core), rhs: 4 (over z).
Axes of the slice: x: 2, y: 2, z: 4, core: 2. Of those that a mesh axis runs over, the one named last changes fastest.
Arguments:
- rhs_vectors: float32 [64, 16, 384], P('patch', 'rhs'), may hold values from -8 to 8
- near_blocks: bfloat16 [64, 4, 384, 384], P('patch'), may hold values from -1 to 5, as said below
- neighbours: int32 [64, 4], P('patch'), may hold values from 0 to 63, as said below
- up_maps: float32 [64, 64, 384], P('patch'), may hold values from -0.3125 to 0.3125
- shift_up: float32 [64, 64, 64], P('patch'), may hold values from -0.25 to 0.25
- far_lists: int32 [8, 4], P('patch'), may hold values from 0 to 7, as said below
- translations: float32 [8, 4, 64, 64], P('patch'), may hold values from -0.375 to 0.375
- shift_down: float32 [64, 64, 64], P('patch'), may hold values from -0.75 to 0.75
- down_maps: float32 [64, 384, 64], P('patch'), may hold values from -0.375 to 0.375
Outputs:
- solution: float32 [64, 16, 384], P('patch', 'rhs')
- residual: float32 [64, 16, 384], P('patch', 'rhs')
The draws below stay inside these ranges and needn't reach their ends.
Inputs may be any that keep to these rules, and one draw needn't show every extreme that they name: `neighbours`: entry 0 of each row is the patch itself; every other entry names a patch of the same cell or of the cell just before or just after it, cyclically. `far_lists`: entry 0 of each row names the cell just before or just after the row's own cell, cyclically, and for cell 0 the cell just before it; every other entry names a cell other than the row's own. `near_blocks`: the blocks keep the operator's symmetric part positive definite.
All inputs are finite; a program needn't handle non-finite values.
Results may differ from the reference program's by a relative error of at most 0.008.
The reference program's roundings to bfloat16 on the way (of `rounded`) count: a program that leaves them out, or rounds other values in their place, can miss the bound.
Values may be sent and summed in bfloat16 or wider, within the bound.
A program may use at most 64 MiB of HBM per device.

```python
import math
import jax
import jax.numpy as jnp
from jax import lax

K = 16
W = 384
E = 64
NB = 4
FL = 4
ITERS = 2
PD = 8
PATCHES = 64
CELLS = 8


def draw_near_blocks(key, part):
    spread = 0.35 / math.sqrt(W * NB)
    noise = jax.random.normal(key, (PATCHES, NB, W, W), jnp.float32) * spread
    selfpart = (jnp.arange(NB) == 0).astype(jnp.float32)[:, None, None] * jnp.eye(W, dtype=jnp.float32) * 4.0
    return (noise + selfpart[None]).astype(jnp.bfloat16)


def draw_neighbours(key, part):
    labels = jnp.arange(PATCHES, dtype=jnp.int32)
    owner = labels // PD
    offset = jax.random.randint(jax.random.fold_in(key, 11), (PATCHES, NB), 0, 3 * PD, dtype=jnp.int32) - PD
    chosen = jnp.mod(owner[:, None] * PD + offset, PATCHES).astype(jnp.int32)
    return chosen.at[:, 0].set(labels)


def draw_far_lists(key, part):
    labels = jnp.arange(CELLS, dtype=jnp.int32)
    offset = jax.random.randint(jax.random.fold_in(key, 23), (CELLS, FL), 1, CELLS, dtype=jnp.int32)
    side = jax.random.randint(jax.random.fold_in(key, 29), (CELLS,), 0, 2, dtype=jnp.int32) * 2 - 1
    side = jnp.where(labels == 0, -1, side).astype(jnp.int32)
    offset = offset.at[:, 0].set(side)
    return jnp.mod(labels[:, None] + offset, CELLS).astype(jnp.int32)


def level_of(key, dims, cuts, low, high):
    gain, own = 1.0, jax.random.fold_in(key, 6)
    for position, shards_of in cuts:
        steps = jnp.exp(jax.random.uniform(jax.random.fold_in(own, position), (shards_of,), jnp.float32, low / len(cuts), high / len(cuts)))
        gain = gain * jnp.repeat(steps, dims[position] // shards_of).reshape([-1 if axis == position else 1 for axis in range(len(dims))])
    return gain


def normal_values(rng, extent, deviation, bound, split=(), kind=jnp.bfloat16):
    loudness = level_of(rng, extent, split, -0.22, 0.18) if split else 1.0
    drawn = jax.random.normal(rng, extent, jnp.float32) * deviation * loudness
    return jnp.minimum(jnp.maximum(drawn, -bound), bound).astype(kind)


def setup_inputs(seed: int = 0) -> dict:
    seeds = jax.random.split(jax.random.key(seed), 10)
    return {
        "rhs_vectors": normal_values(seeds[0], (PATCHES, K, W), 2.0, 8.0, ((0, 8), (1, 4)), jnp.float32),
        "near_blocks": draw_near_blocks(jax.random.fold_in(seeds[9], 71), 0),
        "neighbours": draw_neighbours(jax.random.fold_in(seeds[9], 71), 0),
        "up_maps": normal_values(seeds[3], (PATCHES, E, W), W ** -0.5, 0.3125, ((0, 8),), jnp.float32),
        "shift_up": normal_values(seeds[4], (PATCHES, E, E), (E * PD) ** -0.5, 0.25, ((0, 8),), jnp.float32),
        "far_lists": draw_far_lists(jax.random.fold_in(seeds[9], 71), 0),
        "translations": normal_values(seeds[6], (CELLS, FL, E, E), (E * FL) ** -0.5, 0.375, ((0, 8),), jnp.float32),
        "shift_down": normal_values(seeds[7], (PATCHES, E, E), E ** -0.5, 0.75, ((0, 8),), jnp.float32),
        "down_maps": normal_values(seeds[8], (PATCHES, W, E), (4 * E) ** -0.5, 0.375, ((0, 8),), jnp.float32),
    }


HIGH = lax.Precision.HIGHEST

def spd_solve(matrix, right):
    factor = jnp.linalg.cholesky(matrix)
    return jax.scipy.linalg.cho_solve((factor, True), right)

def gram(left, right):
    return jnp.einsum('pkw,plw->kl', left, right, precision=HIGH)

def mix(field, coeffs):
    return jnp.einsum('pkw,kl->plw', field, coeffs, precision=HIGH)

def operator(field, near_blocks, neighbours, up_maps, shift_up, far_lists, translations, shift_down, down_maps):
    rounded = lax.optimization_barrier(field.astype(jnp.bfloat16)).astype(jnp.float32)
    picked = rounded[neighbours]
    near = jnp.einsum('pjvw,pjkw->pkv', near_blocks.astype(jnp.float32), picked, precision=HIGH)
    moments = jnp.einsum('pew,pkw->pke', up_maps, field, precision=HIGH)
    cells = moments.reshape(CELLS, PD, K, E)
    shifts = shift_up.reshape(CELLS, PD, E, E)
    cell_moment = jnp.einsum('cpfe,cpke->ckf', shifts, cells, precision=HIGH)
    sources = cell_moment[far_lists]
    local_exp = jnp.einsum('cjfe,cjke->ckf', translations, sources, precision=HIGH)
    spread = jnp.repeat(local_exp, PD, axis=0)
    patch_exp = jnp.einsum('pfe,pke->pkf', shift_down, spread, precision=HIGH)
    far = jnp.einsum('pvf,pkf->pkv', down_maps, patch_exp, precision=HIGH)
    return near + far

def reference(rhs_vectors, near_blocks, neighbours, up_maps, shift_up, far_lists, translations, shift_down, down_maps):
    residual = rhs_vectors
    solution = jnp.zeros_like(residual)
    direction = residual
    current = gram(residual, residual)
    for step in range(ITERS):
        image = operator(direction, near_blocks, neighbours, up_maps, shift_up, far_lists, translations, shift_down, down_maps)
        curve = gram(direction, image)
        curve = 0.5 * (curve + curve.T)
        alpha = spd_solve(curve, current)
        solution = solution + mix(direction, alpha)
        residual = residual - mix(image, alpha)
        if step + 1 < ITERS:
            following = gram(residual, residual)
            beta = spd_solve(current, following)
            direction = residual + mix(direction, beta)
            current = following
    return (solution, residual)
```

```python
import functools

import jax
import jax.numpy as jnp
from jax import lax
from jax.experimental import pallas as pl
from jax.experimental.pallas import tpu as pltpu
from jax.sharding import PartitionSpec as P

ITERS = 2
HIGH = lax.Precision.HIGHEST
MESH = pl.DeviceIdType.MESH


def nt(a, b, precision=HIGH):
    return lax.dot_general(
        a, b, (((1,), (1,)), ((), ())), precision=precision, preferred_element_type=jnp.float32
    )


def nn(a, b):
    return lax.dot_general(
        a, b, (((1,), (0,)), ((), ())), precision=HIGH, preferred_element_type=jnp.float32
    )


def eliminate(systems):
    n = systems[0].shape[0]
    for k in range(n):
        done = []
        for a in systems:
            rows = lax.broadcasted_iota(jnp.int32, a.shape, 0)
            row = a[k : k + 1, :] / a[k : k + 1, k : k + 1]
            done.append(jnp.where(rows == k, row, a - a[:, k : k + 1] * row))
        systems = done
    return systems


def kernel(
    cells,
    zs,
    rhs,
    near_hbm,
    neigh,
    up_hbm,
    su_hbm,
    far,
    tr_hbm,
    sd_hbm,
    dn_hbm,
    sol_out,
    res_out,
    blocks,
    up,
    su,
    tr,
    sd,
    dn,
    halo,
    moment,
    mom_out,
    own_dir,
    own_img,
    own_res,
    gathered,
    images,
    full_r,
    full_i,
    full_d,
    strip_out,
    strips,
    new_out,
    news,
    near_sem,
    map_sem,
    halo_s,
    halo_r,
    mom_s,
    mom_r,
    gat_s,
    gat_r,
    img_s,
    img_r,
    strip_s,
    strip_r,
    new_s,
    new_r,
):
    c = lax.axis_index("patch")
    z = lax.axis_index("rhs")
    patches, cols, width = rhs.shape
    terms = su.shape[1]
    total_cols = cols * zs
    total = patches * cells
    devices = cells * zs
    me = c * zs + z

    maps = [(up_hbm, up), (su_hbm, su), (sd_hbm, sd), (dn_hbm, dn), (tr_hbm, tr)]
    map_copies = [
        pltpu.make_async_copy(src, dst, map_sem.at[i]) for i, (src, dst) in enumerate(maps)
    ]
    for copy in map_copies[:2]:
        copy.start()

    barrier = pltpu.get_barrier_semaphore()

    def greet(i, carry):
        other = lax.rem(me + i, devices)
        pl.semaphore_signal(
            barrier, inc=1, device_id=(other // zs, lax.rem(other, zs)), device_id_type=MESH
        )
        return carry

    lax.fori_loop(1, devices, greet, 0)

    def near_copy(p):
        return pltpu.make_async_copy(near_hbm.at[p], blocks.at[p], near_sem.at[p])

    def start_near(p, carry):
        near_copy(p).start()
        return carry

    lax.fori_loop(0, patches, start_near, 0)
    for copy in map_copies[2:]:
        copy.start()

    def cell_of(i):
        return lax.rem(c + i, cells)

    def halo_copy(it, src, side):
        target = cell_of(1 if side == 0 else cells - 1)
        dst = halo.at[it, pl.ds(0 if side == 0 else 2 * patches, patches)]
        return pltpu.make_async_remote_copy(
            src_ref=src,
            dst_ref=dst,
            send_sem=halo_s.at[it, side],
            recv_sem=halo_r.at[it, side],
            device_id=(target, z),
            device_id_type=MESH,
        )

    def moment_copy(it, target, slot):
        return pltpu.make_async_remote_copy(
            src_ref=mom_out.at[it],
            dst_ref=moment.at[it, slot],
            send_sem=mom_s.at[it, target],
            recv_sem=mom_r.at[it, slot],
            device_id=(target, z),
            device_id_type=MESH,
        )

    def z_copy(src, buf, ssem, rsem, target, slot):
        return pltpu.make_async_remote_copy(
            src_ref=src,
            dst_ref=buf.at[slot],
            send_sem=ssem.at[target],
            recv_sem=rsem.at[slot],
            device_id=(c, target),
            device_id_type=MESH,
        )

    def strip_copy(it, target, slot):
        return pltpu.make_async_remote_copy(
            src_ref=strip_out.at[it],
            dst_ref=strips.at[it, slot],
            send_sem=strip_s.at[it, target],
            recv_sem=strip_r.at[it, slot],
            device_id=(target // zs, lax.rem(target, zs)),
            device_id_type=MESH,
        )

    def new_copy(target, slot):
        return pltpu.make_async_remote_copy(
            src_ref=new_out,
            dst_ref=news.at[slot],
            send_sem=new_s.at[target],
            recv_sem=new_r.at[slot],
            device_id=(target, z),
            device_id_type=MESH,
        )

    def others(count, mine, body):
        def step(i, carry):
            body(lax.rem(mine + i, count))
            return carry

        lax.fori_loop(1, count, step, 0)

    def cell_moment(it, src):
        acc = jnp.zeros((cols, terms), jnp.float32)
        for p in range(patches):
            acc = acc + nt(nt(src[p], up[p]), su[p])
        mom_out[it, :, :] = jnp.zeros(mom_out.shape[1:], jnp.float32)
        mom_out[it, :, 0:terms] = acc

    def apply_operator(it):
        halo_copy(it, own_dir, 0).wait_recv()
        halo_copy(it, own_dir, 1).wait_recv()
        first = c * patches - patches

        def near(p, carry):
            if it == 0:
                near_copy(p).wait()
            acc = jnp.zeros((cols, width), jnp.float32)
            for j in range(neigh.shape[1]):
                if j == 0:
                    x = halo[it, patches + p]
                else:
                    spot = jnp.minimum(lax.rem(neigh[p, j] - first + total, total), 3 * patches - 1)
                    x = halo[it, spot]
                acc = acc + nt(x.astype(jnp.bfloat16), blocks[p, j], None)
            own_img[it, p] = acc
            return carry

        lax.fori_loop(0, patches, near, 0)
        others(cells, c, lambda s: moment_copy(it, s, s).wait_recv())
        if it == 0:
            for copy in map_copies[2:]:
                copy.wait()
        local = jnp.zeros((cols, terms), jnp.float32)
        for j in range(far.shape[1]):
            local = local + nt(moment[it, far[0, j]][:, 0:terms], tr[0, j])
        for p in range(patches):
            own_img[it, p] += nt(nt(local, sd[p]), dn[p])

    def assemble(full, buf):
        for p in range(patches):
            for s in range(zs):
                full[p, s * cols : (s + 1) * cols, :] = buf[s, p]

    map_copies[0].wait()
    map_copies[1].wait()
    cell_moment(0, rhs)
    halo[0, pl.ds(patches, patches)] = rhs[...]
    gathered[z] = rhs[...]
    pl.semaphore_wait(barrier, devices - 1)
    halo_copy(0, rhs, 0).start()
    halo_copy(0, rhs, 1).start()
    others(cells, c, lambda t: moment_copy(0, t, c).start())
    others(zs, z, lambda t: z_copy(rhs, gathered, gat_s, gat_r, t, z).start())

    sel = (
        lax.broadcasted_iota(jnp.int32, (cols, total_cols), 1)
        == lax.broadcasted_iota(jnp.int32, (cols, total_cols), 0) + z * cols
    ).astype(jnp.float32)
    eye = (
        lax.broadcasted_iota(jnp.int32, (total_cols, total_cols), 1)
        == lax.broadcasted_iota(jnp.int32, (total_cols, total_cols), 0)
    ).astype(jnp.float32)

    def share_strips(it, direction, with_rr):
        acc = jnp.zeros((cols, total_cols), jnp.float32)
        cur = jnp.zeros((cols, total_cols), jnp.float32)
        for p in range(patches):
            acc = acc + nt(own_img[it, p], direction[p])
            if with_rr:
                cur = cur + nt(rhs[p], direction[p])
        strip_out[it, 0, :, 0:total_cols] = acc
        strip_out[it, 1, :, 0:total_cols] = cur
        strips[it, me] = strip_out[it]
        others(devices, me, lambda t: strip_copy(it, t, me).start())

    def collect_strips(it):
        others(devices, me, lambda s: strip_copy(it, s, s).wait_recv())
        curve, cur = [], []
        for s in range(zs):
            acc = strips[it, s]
            for k in range(1, cells):
                acc = acc + strips[it, k * zs + s]
            curve.append(acc[0, :, 0:total_cols])
            cur.append(acc[1, :, 0:total_cols])
        curve = jnp.concatenate(curve, axis=0)
        cur = jnp.concatenate(cur, axis=0)
        return 0.5 * (curve + nt(eye, curve)), cur

    apply_operator(0)
    others(zs, z, lambda t: z_copy(own_img.at[0], images.at[0], img_s.at[0], img_r.at[0], t, z).start())
    images[0, z] = own_img[0]
    others(zs, z, lambda s: z_copy(rhs, gathered, gat_s, gat_r, s, s).wait_recv())
    assemble(full_r, gathered)
    share_strips(0, full_r, True)
    curve, current = collect_strips(0)
    solved, inverse = eliminate(
        [jnp.concatenate([curve, current], axis=1), jnp.concatenate([current, eye], axis=1)]
    )
    alpha_t = nt(eye, solved[:, total_cols:])
    inverse = inverse[:, total_cols:]
    alpha_own = nn(sel, alpha_t)
    others(
        zs,
        z,
        lambda s: z_copy(own_img.at[0], images.at[0], img_s.at[0], img_r.at[0], s, s).wait_recv(),
    )
    assemble(full_i, images.at[0])
    new = jnp.zeros((total_cols, total_cols), jnp.float32)
    for p in range(patches):
        r1 = full_r[p] - nn(alpha_t, full_i[p])
        full_d[p] = r1
        new = new + nt(r1, r1)
    new_out[:, 0:total_cols] = new
    news[c] = new_out[...]
    others(cells, c, lambda t: new_copy(t, c).start())
    for p in range(patches):
        own_res[p] = rhs[p] - nn(alpha_own, full_i[p])
        sol_out[p] = nn(alpha_own, full_r[p])
    others(cells, c, lambda s: new_copy(s, s).wait_recv())
    new = news[0]
    for k in range(1, cells):
        new = new + news[k]
    new = new[:, 0:total_cols]
    beta = nn(inverse, new)
    beta_t = nt(eye, beta)
    beta_own = nn(sel, beta_t)
    for p in range(patches):
        own_dir[p] = own_res[p] + nn(beta_own, full_r[p])
    halo_copy(1, own_dir, 0).start()
    halo_copy(1, own_dir, 1).start()
    cell_moment(1, own_dir)
    others(cells, c, lambda t: moment_copy(1, t, c).start())
    halo[1, pl.ds(patches, patches)] = own_dir[...]
    for p in range(patches):
        full_d[p] += nn(beta_t, full_r[p])

    apply_operator(1)
    others(zs, z, lambda t: z_copy(own_img.at[1], images.at[1], img_s.at[1], img_r.at[1], t, z).start())
    images[1, z] = own_img[1]
    share_strips(1, full_d, False)
    curve, _ = collect_strips(1)
    (solved,) = eliminate([jnp.concatenate([curve, new], axis=1)])
    alpha_t = nt(eye, solved[:, total_cols:])
    alpha_own = nn(sel, alpha_t)
    for p in range(patches):
        sol_out[p] += nn(alpha_own, full_d[p])
    others(
        zs,
        z,
        lambda s: z_copy(own_img.at[1], images.at[1], img_s.at[1], img_r.at[1], s, s).wait_recv(),
    )
    assemble(full_i, images.at[1])
    for p in range(patches):
        res_out[p] = own_res[p] - nn(alpha_own, full_i[p])

    for it in range(ITERS):
        halo_copy(it, own_dir, 0).wait_send()
        halo_copy(it, own_dir, 1).wait_send()
        others(cells, c, lambda t: moment_copy(it, t, c).wait_send())
        others(devices, me, lambda t: strip_copy(it, t, me).wait_send())
        others(
            zs,
            z,
            lambda t: z_copy(
                own_img.at[it], images.at[it], img_s.at[it], img_r.at[it], t, z
            ).wait_send(),
        )
    others(zs, z, lambda t: z_copy(rhs, gathered, gat_s, gat_r, t, z).wait_send())
    others(cells, c, lambda t: new_copy(t, c).wait_send())


def on_device(cells, zs, *args):
    rhs, near, neigh, up, su, far, tr, sd, dn = args
    patches, cols, width = rhs.shape
    full = cols * zs
    devices = cells * zs
    f32 = jnp.float32
    vmem = pl.BlockSpec(memory_space=pltpu.VMEM)
    smem = pl.BlockSpec(memory_space=pltpu.SMEM)
    hbm = pl.BlockSpec(memory_space=pl.ANY)
    dma = pltpu.SemaphoreType.DMA
    out = pl.pallas_call(
        functools.partial(kernel, cells, zs),
        out_shape=[jax.ShapeDtypeStruct(rhs.shape, f32)] * 2,
        in_specs=[vmem, hbm, smem, hbm, hbm, smem, hbm, hbm, hbm],
        out_specs=[vmem, vmem],
        scratch_shapes=[
            pltpu.VMEM(near.shape, near.dtype),
            pltpu.VMEM(up.shape, f32),
            pltpu.VMEM(su.shape, f32),
            pltpu.VMEM(tr.shape, f32),
            pltpu.VMEM(sd.shape, f32),
            pltpu.VMEM(dn.shape, f32),
            pltpu.VMEM((ITERS, 3 * patches, cols, width), f32),
            pltpu.VMEM((ITERS, cells, cols, 128), f32),
            pltpu.VMEM((ITERS, cols, 128), f32),
            pltpu.VMEM(rhs.shape, f32),
            pltpu.VMEM((ITERS,) + rhs.shape, f32),
            pltpu.VMEM(rhs.shape, f32),
            pltpu.VMEM((zs,) + rhs.shape, f32),
            pltpu.VMEM((ITERS, zs) + rhs.shape, f32),
            pltpu.VMEM((patches, full, width), f32),
            pltpu.VMEM((patches, full, width), f32),
            pltpu.VMEM((patches, full, width), f32),
            pltpu.VMEM((ITERS, 2, cols, 128), f32),
            pltpu.VMEM((ITERS, devices, 2, cols, 128), f32),
            pltpu.VMEM((full, 128), f32),
            pltpu.VMEM((cells, full, 128), f32),
            dma((patches,)),
            dma((5,)),
            dma((ITERS, 2)),
            dma((ITERS, 2)),
            dma((ITERS, cells)),
            dma((ITERS, cells)),
            dma((zs,)),
            dma((zs,)),
            dma((ITERS, zs)),
            dma((ITERS, zs)),
            dma((ITERS, devices)),
            dma((ITERS, devices)),
            dma((cells,)),
            dma((cells,)),
        ],
        compiler_params=pltpu.CompilerParams(
            collective_id=0, has_side_effects=True, vmem_limit_bytes=48 * 1024 * 1024
        ),
        name="block_cg",
    )(rhs, near, neigh, up, su, far, tr, sd, dn)
    return tuple(out)


def solution(mesh):
    cells = mesh.shape["patch"]
    zs = mesh.shape["rhs"]
    return jax.shard_map(
        functools.partial(on_device, cells, zs),
        mesh=mesh,
        in_specs=(
            P("patch", "rhs", None),
            P("patch", None, None, None),
            P("patch", None),
            P("patch", None, None),
            P("patch", None, None),
            P("patch", None),
            P("patch", None, None, None),
            P("patch", None, None),
            P("patch", None, None),
        ),
        out_specs=(P("patch", "rhs", None), P("patch", "rhs", None)),
        check_vma=False,
    )
```

```python
import functools

import jax
import jax.numpy as jnp
from jax import lax
from jax.experimental import pallas as pl
from jax.experimental.pallas import tpu as pltpu
from jax.sharding import PartitionSpec as P

ITERS = 2
HIGH = lax.Precision.HIGHEST
MESH = pl.DeviceIdType.MESH


def nt(a, b, precision=HIGH):
    return lax.dot_general(
        a, b, (((1,), (1,)), ((), ())), precision=precision, preferred_element_type=jnp.float32
    )


def nn(a, b):
    return lax.dot_general(
        a, b, (((1,), (0,)), ((), ())), precision=HIGH, preferred_element_type=jnp.float32
    )


def split(x):
    high = x.astype(jnp.bfloat16)
    return high, (x - high.astype(jnp.float32)).astype(jnp.bfloat16)


def eliminate(systems):
    n = systems[0].shape[0]
    for k in range(n):
        done = []
        for a in systems:
            rows = lax.broadcasted_iota(jnp.int32, a.shape, 0)
            row = a[k : k + 1, :] / a[k : k + 1, k : k + 1]
            done.append(jnp.where(rows == k, row, a - a[:, k : k + 1] * row))
        systems = done
    return systems


def kernel(
    cells,
    zs,
    rhs,
    near_hbm,
    neigh,
    up_hbm,
    su_hbm,
    far,
    tr_hbm,
    sd_hbm,
    dn_hbm,
    sol_out,
    res_out,
    blocks,
    up,
    su,
    tr,
    sd,
    dn,
    gcat,
    ucat,
    halo,
    moment,
    mom_out,
    own_dir,
    own_img,
    own_res,
    gathered,
    images,
    full_r,
    full_i,
    full_d,
    strip_out,
    strips,
    new_out,
    news,
    near_sem,
    map_sem,
    halo_s,
    halo_r,
    mom_s,
    mom_r,
    gat_s,
    gat_r,
    img_s,
    img_r,
    strip_s,
    strip_r,
    new_s,
    new_r,
):
    c = lax.axis_index("patch")
    z = lax.axis_index("rhs")
    patches, cols, width = rhs.shape
    terms = su.shape[1]
    total_cols = cols * zs
    total = patches * cells
    devices = cells * zs
    me = c * zs + z

    maps = [(up_hbm, up), (su_hbm, su), (sd_hbm, sd), (dn_hbm, dn), (tr_hbm, tr)]
    map_copies = [
        pltpu.make_async_copy(src, dst, map_sem.at[i]) for i, (src, dst) in enumerate(maps)
    ]
    for copy in map_copies[:2]:
        copy.start()

    barrier = pltpu.get_barrier_semaphore()

    def greet(i, carry):
        other = lax.rem(me + i, devices)
        pl.semaphore_signal(
            barrier, inc=1, device_id=(other // zs, lax.rem(other, zs)), device_id_type=MESH
        )
        return carry

    lax.fori_loop(1, devices, greet, 0)

    def near_copy(p):
        return pltpu.make_async_copy(near_hbm.at[p], blocks.at[p], near_sem.at[p])

    def start_near(p, carry):
        near_copy(p).start()
        return carry

    lax.fori_loop(0, patches, start_near, 0)
    for copy in map_copies[2:]:
        copy.start()

    def cell_of(i):
        return lax.rem(c + i, cells)

    def halo_copy(it, src, side):
        target = cell_of(1 if side == 0 else cells - 1)
        dst = halo.at[it, pl.ds(0 if side == 0 else 2 * patches, patches)]
        return pltpu.make_async_remote_copy(
            src_ref=src,
            dst_ref=dst,
            send_sem=halo_s.at[it, side],
            recv_sem=halo_r.at[it, side],
            device_id=(target, z),
            device_id_type=MESH,
        )

    def moment_copy(it, target, slot):
        return pltpu.make_async_remote_copy(
            src_ref=mom_out.at[it],
            dst_ref=moment.at[it, slot],
            send_sem=mom_s.at[it, target],
            recv_sem=mom_r.at[it, slot],
            device_id=(target, z),
            device_id_type=MESH,
        )

    def z_copy(src, buf, ssem, rsem, target, slot):
        return pltpu.make_async_remote_copy(
            src_ref=src,
            dst_ref=buf.at[slot],
            send_sem=ssem.at[target],
            recv_sem=rsem.at[slot],
            device_id=(c, target),
            device_id_type=MESH,
        )

    def strip_copy(it, target, slot):
        return pltpu.make_async_remote_copy(
            src_ref=strip_out.at[it],
            dst_ref=strips.at[it, slot],
            send_sem=strip_s.at[it, target],
            recv_sem=strip_r.at[it, slot],
            device_id=(target // zs, lax.rem(target, zs)),
            device_id_type=MESH,
        )

    def new_copy(target, slot):
        return pltpu.make_async_remote_copy(
            src_ref=new_out,
            dst_ref=news.at[slot],
            send_sem=new_s.at[target],
            recv_sem=new_r.at[slot],
            device_id=(target, z),
            device_id_type=MESH,
        )

    def others(count, mine, body):
        def step(i, carry):
            body(lax.rem(mine + i, count))
            return carry

        lax.fori_loop(1, count, step, 0)

    def cell_moment(it, src):
        acc = jnp.zeros((cols, terms), jnp.float32)
        for p in range(patches):
            acc = acc + nt(nt(src[p], up[p]), su[p])
        mom_out[it, :, :] = jnp.zeros(mom_out.shape[1:], jnp.float32)
        mom_out[it, :, 0:terms] = acc

    def apply_operator(it):
        halo_copy(it, own_dir, 0).wait_recv()
        halo_copy(it, own_dir, 1).wait_recv()
        first = c * patches - patches

        def near(p, carry):
            if it == 0:
                near_copy(p).wait()
            acc = jnp.zeros((cols, width), jnp.float32)
            for j in range(neigh.shape[0]):
                if j == 0:
                    x = halo[it, patches + p]
                else:
                    spot = jnp.minimum(lax.rem(neigh[j, p] - first + total, total), 3 * patches - 1)
                    x = halo[it, spot]
                acc = acc + nt(x.astype(jnp.bfloat16), blocks[p, j], None)
            own_img[it, p] = acc
            return carry

        for p in range(patches):
            near(p, 0)
        others(cells, c, lambda s: moment_copy(it, s, s).wait_recv())
        local = jnp.zeros((cols, terms), jnp.float32)
        for j in range(far.shape[1]):
            local = local + nt(moment[it, far[0, j]][:, 0:terms], tr[0, j])
        high, low = split(local)
        local = jnp.concatenate(
            [high.astype(jnp.float32), high.astype(jnp.float32), low.astype(jnp.float32)], axis=1
        ).astype(jnp.bfloat16)
        for p in range(patches):
            own_img[it, p] += jnp.dot(local, gcat[p], preferred_element_type=jnp.float32)

    def assemble(full, buf):
        for p in range(patches):
            for s in range(zs):
                full[p, s * cols : (s + 1) * cols, :] = buf[s, p]

    map_copies[0].wait()
    map_copies[1].wait()
    cell_moment(0, rhs)
    halo[0, pl.ds(patches, patches)] = rhs[...]
    gathered[z] = rhs[...]
    pl.semaphore_wait(barrier, devices - 1)
    halo_copy(0, rhs, 0).start()
    halo_copy(0, rhs, 1).start()
    others(cells, c, lambda t: moment_copy(0, t, c).start())
    others(zs, z, lambda t: z_copy(rhs, gathered, gat_s, gat_r, t, z).start())

    for copy in map_copies[2:]:
        copy.wait()
    for p in range(patches):
        both = lax.dot_general(
            sd[p],
            dn[p],
            (((0,), (0,)), ((), ())),
            precision=HIGH,
            preferred_element_type=jnp.float32,
        )
        high, low = split(both)
        gcat[p, 0:terms, :] = high
        gcat[p, terms : 2 * terms, :] = low
        gcat[p, 2 * terms : 3 * terms, :] = high

    def combine_up():
        for p in range(patches):
            high, low = split(nn(su[p], up[p]))
            ucat[p, 0:terms, :] = high
            ucat[p, terms : 2 * terms, :] = low

    def later_moment(it, src):
        acc = jnp.zeros((2 * cols, 2 * terms), jnp.float32)
        for p in range(patches):
            high, low = split(src[p])
            x = jnp.concatenate([high.astype(jnp.float32), low.astype(jnp.float32)], axis=0)
            acc = acc + nt(x.astype(jnp.bfloat16), ucat[p], None)
        acc = acc[:, 0:terms] + acc[:, terms:]
        mom_out[it, :, :] = jnp.zeros(mom_out.shape[1:], jnp.float32)
        mom_out[it, :, 0:terms] = acc[0:cols] + acc[cols:]

    sel = (
        lax.broadcasted_iota(jnp.int32, (cols, total_cols), 1)
        == lax.broadcasted_iota(jnp.int32, (cols, total_cols), 0) + z * cols
    ).astype(jnp.float32)
    eye = (
        lax.broadcasted_iota(jnp.int32, (total_cols, total_cols), 1)
        == lax.broadcasted_iota(jnp.int32, (total_cols, total_cols), 0)
    ).astype(jnp.float32)

    def share_strips(it, direction, with_rr):
        acc = jnp.zeros(((2 if with_rr else 1) * cols, total_cols), jnp.float32)
        for p in range(patches):
            left = own_img[it, p]
            if with_rr:
                left = jnp.concatenate([left, rhs[p]], axis=0)
            acc = acc + nt(left, direction[p])
        if with_rr:
            acc = jnp.concatenate([acc[0:cols], acc[cols:]], axis=1)
        strip_out[it, :, 0 : acc.shape[1]] = acc
        strips[it, me] = strip_out[it]
        others(devices, me, lambda t: strip_copy(it, t, me).start())

    def collect_strips(it):
        others(devices, me, lambda s: strip_copy(it, s, s).wait_recv())
        curve, cur = [], []
        for s in range(zs):
            acc = strips[it, s]
            for k in range(1, cells):
                acc = acc + strips[it, k * zs + s]
            curve.append(acc[:, 0:total_cols])
            cur.append(acc[:, total_cols : 2 * total_cols])
        curve = jnp.concatenate(curve, axis=0)
        cur = jnp.concatenate(cur, axis=0)
        return 0.5 * (curve + nt(eye, curve)), cur

    apply_operator(0)
    others(zs, z, lambda s: z_copy(rhs, gathered, gat_s, gat_r, s, s).wait_recv())
    assemble(full_r, gathered)
    share_strips(0, full_r, True)
    others(zs, z, lambda t: z_copy(own_img.at[0], images.at[0], img_s.at[0], img_r.at[0], t, z).start())
    images[0, z] = own_img[0]
    combine_up()
    curve, current = collect_strips(0)
    solved, inverse = eliminate(
        [jnp.concatenate([curve, current], axis=1), jnp.concatenate([current, eye], axis=1)]
    )
    alpha_t = nt(eye, solved[:, total_cols:])
    inverse = inverse[:, total_cols:]
    alpha_own = nn(sel, alpha_t)
    others(
        zs,
        z,
        lambda s: z_copy(own_img.at[0], images.at[0], img_s.at[0], img_r.at[0], s, s).wait_recv(),
    )
    assemble(full_i, images.at[0])
    new = jnp.zeros((total_cols, total_cols), jnp.float32)
    for p in range(patches):
        r1 = full_r[p] - nn(alpha_t, full_i[p])
        full_d[p] = r1
        new = new + nt(r1, r1)
    new_out[:, 0:total_cols] = new
    news[c] = new_out[...]
    others(cells, c, lambda t: new_copy(t, c).start())
    for p in range(patches):
        own_res[p] = rhs[p] - nn(alpha_own, full_i[p])
        sol_out[p] = nn(alpha_own, full_r[p])
    others(cells, c, lambda s: new_copy(s, s).wait_recv())
    new = news[0]
    for k in range(1, cells):
        new = new + news[k]
    new = new[:, 0:total_cols]
    beta = nn(inverse, new)
    beta_t = nt(eye, beta)
    beta_own = nn(sel, beta_t)
    for p in range(patches):
        own_dir[p] = own_res[p] + nn(beta_own, full_r[p])
    halo_copy(1, own_dir, 0).start()
    halo_copy(1, own_dir, 1).start()
    later_moment(1, own_dir)
    others(cells, c, lambda t: moment_copy(1, t, c).start())
    halo[1, pl.ds(patches, patches)] = own_dir[...]
    for p in range(patches):
        full_d[p] += nn(beta_t, full_r[p])

    apply_operator(1)
    share_strips(1, full_d, False)
    others(zs, z, lambda t: z_copy(own_img.at[1], images.at[1], img_s.at[1], img_r.at[1], t, z).start())
    images[1, z] = own_img[1]
    curve, _ = collect_strips(1)
    (solved,) = eliminate([jnp.concatenate([curve, new], axis=1)])
    alpha_t = nt(eye, solved[:, total_cols:])
    alpha_own = nn(sel, alpha_t)
    for p in range(patches):
        sol_out[p] += nn(alpha_own, full_d[p])
    others(
        zs,
        z,
        lambda s: z_copy(own_img.at[1], images.at[1], img_s.at[1], img_r.at[1], s, s).wait_recv(),
    )
    assemble(full_i, images.at[1])
    for p in range(patches):
        res_out[p] = own_res[p] - nn(alpha_own, full_i[p])

    for it in range(ITERS):
        halo_copy(it, own_dir, 0).wait_send()
        halo_copy(it, own_dir, 1).wait_send()
        others(cells, c, lambda t: moment_copy(it, t, c).wait_send())
        others(devices, me, lambda t: strip_copy(it, t, me).wait_send())
        others(
            zs,
            z,
            lambda t: z_copy(
                own_img.at[it], images.at[it], img_s.at[it], img_r.at[it], t, z
            ).wait_send(),
        )
    others(zs, z, lambda t: z_copy(rhs, gathered, gat_s, gat_r, t, z).wait_send())
    others(cells, c, lambda t: new_copy(t, c).wait_send())


def on_device(cells, zs, *args):
    rhs, near, neigh, up, su, far, tr, sd, dn = args
    patches, cols, width = rhs.shape
    dn = jnp.swapaxes(dn, 1, 2)
    neigh = neigh.T
    full = cols * zs
    devices = cells * zs
    f32 = jnp.float32
    vmem = pl.BlockSpec(memory_space=pltpu.VMEM)
    smem = pl.BlockSpec(memory_space=pltpu.SMEM)
    hbm = pl.BlockSpec(memory_space=pl.ANY)
    dma = pltpu.SemaphoreType.DMA
    out = pl.pallas_call(
        functools.partial(kernel, cells, zs),
        out_shape=[jax.ShapeDtypeStruct(rhs.shape, f32)] * 2,
        in_specs=[vmem, hbm, smem, hbm, hbm, smem, hbm, hbm, hbm],
        out_specs=[vmem, vmem],
        scratch_shapes=[
            pltpu.VMEM(near.shape, near.dtype),
            pltpu.VMEM(up.shape, f32),
            pltpu.VMEM(su.shape, f32),
            pltpu.VMEM(tr.shape, f32),
            pltpu.VMEM(sd.shape, f32),
            pltpu.VMEM(dn.shape, f32),
            pltpu.VMEM((patches, 3 * su.shape[1], width), jnp.bfloat16),
            pltpu.VMEM((patches, 2 * su.shape[1], width), jnp.bfloat16),
            pltpu.VMEM((ITERS, 3 * patches, cols, width), f32),
            pltpu.VMEM((ITERS, cells, cols, 128), f32),
            pltpu.VMEM((ITERS, cols, 128), f32),
            pltpu.VMEM(rhs.shape, f32),
            pltpu.VMEM((ITERS,) + rhs.shape, f32),
            pltpu.VMEM(rhs.shape, f32),
            pltpu.VMEM((zs,) + rhs.shape, f32),
            pltpu.VMEM((ITERS, zs) + rhs.shape, f32),
            pltpu.VMEM((patches, full, width), f32),
            pltpu.VMEM((patches, full, width), f32),
            pltpu.VMEM((patches, full, width), f32),
            pltpu.VMEM((ITERS, cols, 128), f32),
            pltpu.VMEM((ITERS, devices, cols, 128), f32),
            pltpu.VMEM((full, 128), f32),
            pltpu.VMEM((cells, full, 128), f32),
            dma((patches,)),
            dma((5,)),
            dma((ITERS, 2)),
            dma((ITERS, 2)),
            dma((ITERS, cells)),
            dma((ITERS, cells)),
            dma((zs,)),
            dma((zs,)),
            dma((ITERS, zs)),
            dma((ITERS, zs)),
            dma((ITERS, devices)),
            dma((ITERS, devices)),
            dma((cells,)),
            dma((cells,)),
        ],
        compiler_params=pltpu.CompilerParams(
            collective_id=0, has_side_effects=True, vmem_limit_bytes=60 * 1024 * 1024
        ),
        name="block_cg",
    )(rhs, near, neigh, up, su, far, tr, sd, dn)
    return tuple(out)


def solution(mesh):
    cells = mesh.shape["patch"]
    zs = mesh.shape["rhs"]
    return jax.shard_map(
        functools.partial(on_device, cells, zs),
        mesh=mesh,
        in_specs=(
            P("patch", "rhs", None),
            P("patch", None, None, None),
            P("patch", None),
            P("patch", None, None),
            P("patch", None, None),
            P("patch", None),
            P("patch", None, None, None),
            P("patch", None, None),
            P("patch", None, None),
        ),
        out_specs=(P("patch", "rhs", None), P("patch", "rhs", None)),
        check_vma=False,
    )
```
